32 devices in a mesh: dev: 32 (over z, y, x, core).
Axes of the slice: x: 2, y: 2, z: 4, core: 2. Of those that a mesh axis runs over, the one named last changes fastest.
Arguments:
- occurrence: bfloat16 [2048, 128, 128], P('dev'), may hold values from -0.5 to 0.5
- block_owner: int32 [2048, 1], P('dev'), may hold values from 0 to 31; in each aligned block of 64 rows (0 to 63, 64 to 127, ...) at most 4 rows name the same one
- read_block: int32 [2048], P('dev'), may hold values from 0 to 15
- slot_order: int32 [32, 128], P('dev'), may hold values from 0 to 127, each once within a row
Outputs:
- margin: float32 [65536, 512], P('dev')
The draws below stay inside these ranges and needn't reach their ends.
Inputs may be any that keep to these rules, and one draw needn't show every extreme that they name: `block_owner`: among the blocks of one device no owner is named more than 4 times, a bound that some block reaches. `slot_order`: each row names every number of 0 to 127 once.
All inputs are finite; a program needn't handle non-finite values.
Results may differ from the reference program's by a relative error of at most 0.0026.
Values may be sent and summed in bfloat16 or wider, within the bound.
A program may use at most 128 MiB of HBM per device.

```python
import math
import jax
import jax.numpy as jnp
import numpy as np
from jax import lax

RB = 128
KB = 128
CAP = 4
S_DEV = 64
RB_DEV = 16
PAIR_MOST = 4
BLOCKS = 2048
N_DEV = 32


def with_ends(array, stream_key, smallest, high):
    longest = array.shape.index(max(array.shape))
    spots = []
    for shift in (0, 1):
        where = [jax.random.randint(jax.random.fold_in(stream_key, axis), (), 0, length) for axis, length in enumerate(array.shape)]
        where[longest] = (where[longest] + shift) % array.shape[longest]
        spots.append(tuple(where))
    return array.at[spots[0]].set(smallest).at[spots[1]].set(high)


def level_of(own_key, dims, shards, smallest, high):
    gain, own = 1.0, jax.random.fold_in(own_key, 6)
    for axis_at, blocks in shards:
        heights = jnp.exp(jax.random.uniform(jax.random.fold_in(own, axis_at), (blocks,), jnp.float32, smallest / len(shards), high / len(shards)))
        gain = gain * jnp.repeat(heights, dims[axis_at] // blocks).reshape([-1 if axis == axis_at else 1 for axis in range(len(dims))])
    return gain


def shared_out(rng, own, number, rows, count, top, reach, lean):
    sequence = jax.random.permutation(rng, count)
    heavy_load, usual = shares(count, rows * top, reach, lean, True), shares(count, rows * top, reach, lean, False)
    places = jnp.arange(count)

    def named(sizes, turn):
        used = int((sizes > 0).sum())
        fixed = max(1, used // 4)
        moved = fixed + (places - fixed + turn * (used - fixed)) % max(1, count - fixed)
        return jnp.zeros((count,), jnp.int32).at[sequence[jnp.where(places < fixed, places, moved)]].set(jnp.asarray(sizes, jnp.int32))

    sizes = jnp.where(number % 4 == 0, named(heavy_load, number // 4), named(usual, number - number // 4 - 1))
    mixed = jax.random.permutation(jax.random.fold_in(own, 3), count)
    giver, taker = mixed[0:count // 2 * 2:2], mixed[1:count // 2 * 2:2]
    margin = jnp.minimum(sizes[giver] - 1, reach - sizes[taker]) // 2
    margin = jnp.where((giver == sequence[0]) | (taker == sequence[0]) | (sizes[taker] == 0), 0, jnp.maximum(margin, 0))
    moved = jax.random.randint(jax.random.fold_in(own, 4), (count // 2,), 0, 1 << 20) % (margin + 1)
    sizes = sizes.at[giver].add(-moved).at[taker].add(moved)
    labels = jnp.searchsorted(jnp.cumsum(sizes), jnp.arange(rows * top), side="right").astype(jnp.int32)
    table = labels.reshape(top, rows).T
    table = table[jax.random.permutation(jax.random.fold_in(own, 1), rows)]
    turn = jax.random.randint(jax.random.fold_in(own, 2), (rows, 1), 0, top)
    return jnp.take_along_axis(table, (jnp.arange(top)[None, :] + turn) % top, axis=1)


def shares(number_of, total, limit, lean, full):
    portions = [(1 << 20) // math.isqrt(grade ** lean) + 1 for grade in range(1, number_of + 1)]
    largest = limit if full else min(limit, max(-(-total // number_of), total * portions[0] // sum(portions)))
    least = 1 if total - largest >= number_of - 1 else 0
    counts, spare = [largest] + [least] * (number_of - 1), total - largest - least * (number_of - 1)
    while spare > 0:
        candidates = [i for i in range(1, number_of) if counts[i] < largest] or [i for i in range(1, number_of) if counts[i] < limit]
        whole, budget = sum([portions[i] for i in candidates]), spare
        for i in candidates:
            addition = min(limit - counts[i], max(1, budget * portions[i] // whole), spare)
            counts[i] = counts[i] + addition
            spare = spare - addition
    return np.array(counts)


def noise(key, extent, scale, reach, shards=(), held_as=jnp.bfloat16):
    loudness = level_of(key, extent, shards, -0.22, 0.18) if shards else 1.0
    drawn = jax.random.normal(key, extent, jnp.float32) * scale * loudness
    return jnp.minimum(jnp.maximum(drawn, -reach), reach).astype(held_as)


def setup_inputs(seed: int = 0) -> dict:
    arg_keys = jax.random.split(jax.random.key(seed), 5)
    occurrence = noise(arg_keys[0], (BLOCKS, RB, KB), KB ** -0.5, 0.5, ((0, 32),))
    block_owner_keys = jax.random.split(jax.random.fold_in(arg_keys[1], 1), BLOCKS // S_DEV)
    block_owner_turns = jax.random.permutation(jax.random.fold_in(arg_keys[1], 3), BLOCKS // S_DEV)
    block_owner = jax.vmap(lambda own, number: shared_out(jax.random.fold_in(arg_keys[1], 2), own, number, S_DEV, N_DEV, 1, PAIR_MOST, 2))(block_owner_keys, block_owner_turns).reshape((BLOCKS, 1))
    read_block = with_ends(jax.random.randint(arg_keys[2], (BLOCKS,), 0, RB_DEV), jax.random.fold_in(arg_keys[2], 1), 0, RB_DEV - 1).astype(jnp.int32)
    slot_order = jax.vmap(lambda own: jax.random.permutation(own, N_DEV * PAIR_MOST))(jax.random.split(arg_keys[3], N_DEV)).reshape((N_DEV, N_DEV * PAIR_MOST)).astype(jnp.int32)
    return dict(occurrence=occurrence, block_owner=block_owner, read_block=read_block, slot_order=slot_order)


def reference(occurrence, block_owner, read_block, slot_order):
    block_total = occurrence.shape[0]
    slot_total = N_DEV * PAIR_MOST
    owners = block_owner[:, 0].reshape(N_DEV, S_DEV)
    positions = jnp.arange(S_DEV, dtype=jnp.int32)
    earlier = positions[None, :] < positions[:, None]
    same_owner = owners[:, :, None] == owners[:, None, :]
    earlier_count = jnp.sum((same_owner & earlier[None]).astype(jnp.int32), axis=2).astype(jnp.int32)
    source = jnp.arange(N_DEV, dtype=jnp.int32)[:, None]
    slot_index = (source * PAIR_MOST + earlier_count).astype(jnp.int32)
    holder = jnp.full((N_DEV, slot_total), -1, jnp.int32)
    holder = holder.at[owners.reshape(-1), slot_index.reshape(-1)].set(jnp.arange(block_total, dtype=jnp.int32))
    ordered_holder = jnp.take_along_axis(holder, slot_order.astype(jnp.int32), axis=1)
    holder_safe = jnp.maximum(ordered_holder, 0)
    stacked = jnp.where((ordered_holder >= 0)[:, :, None, None], occurrence[holder_safe], jnp.zeros((), occurrence.dtype))
    groups = stacked.reshape(N_DEV, slot_total // CAP, CAP, RB, KB)
    owner_rows = jnp.arange(N_DEV, dtype=jnp.int32)[:, None] + jnp.zeros((1, slot_total), jnp.int32)
    place_of = jnp.zeros((N_DEV, slot_total), jnp.int32)
    place_of = place_of.at[owner_rows, slot_order.astype(jnp.int32)].set(
        jnp.zeros((N_DEV, 1), jnp.int32) + jnp.arange(slot_total, dtype=jnp.int32)[None, :])
    by_source = occurrence.reshape(N_DEV, S_DEV, RB, KB)
    read_rows = read_block.reshape(N_DEV, S_DEV)

    def one_source(carried, source_index):
        own_blocks = by_source[source_index]
        own_owner = owners[source_index]
        own_place = place_of[own_owner, slot_index[source_index]]
        group_blocks = groups[own_owner, own_place // CAP]
        tile_block = jnp.einsum('bik,bjrk->bijr', own_blocks.astype(jnp.float32), group_blocks.astype(jnp.float32))
        tile_block = tile_block.astype(jnp.bfloat16)
        onehot = (read_rows[source_index][None, :] == jnp.arange(RB_DEV, dtype=jnp.int32)[:, None]).astype(jnp.float32)
        summed = jnp.einsum('nb,bijr->nijr', onehot, tile_block.astype(jnp.float32))
        return carried, summed.reshape(RB_DEV * RB, CAP * RB)

    _, per_source = lax.scan(one_source, jnp.zeros((), jnp.float32), jnp.arange(N_DEV, dtype=jnp.int32))
    return per_source.reshape(N_DEV * RB_DEV * RB, CAP * RB)
```

```python
import functools
import jax
import jax.numpy as jnp
import numpy as np
from jax import lax
from jax.experimental import pallas as pl
from jax.experimental.pallas import tpu as pltpu
from jax.sharding import PartitionSpec as P

CAP = 4
RB_DEV = 16
CORES = 2


def exchange_by_owner(occurrence, block_owner, read_block, slot_order):
    devices = lax.axis_size("dev")
    blocks, rows, kmers = occurrence.shape
    per_pair = 2 * blocks // devices
    slot_total = devices * per_pair
    owners = block_owner[:, 0]
    positions = jnp.arange(blocks, dtype=jnp.int32)
    earlier = positions[None, :] < positions[:, None]
    same_owner = owners[:, None] == owners[None, :]
    earlier_count = jnp.sum((same_owner & earlier).astype(jnp.int32), axis=1)
    send_slot = owners * per_pair + earlier_count
    onehot = (send_slot[:, None] == jnp.arange(slot_total, dtype=jnp.int32)[None, :]).astype(
        jnp.bfloat16
    )
    outgoing = jnp.einsum(
        "bs,bik->sik", onehot, occurrence, preferred_element_type=jnp.float32
    ).astype(jnp.bfloat16)
    received = lax.all_to_all(outgoing, "dev", split_axis=0, concat_axis=0, tiled=True)
    order_row = slot_order[0]
    place_of = (
        jnp.zeros((slot_total,), jnp.int32)
        .at[order_row]
        .set(jnp.arange(slot_total, dtype=jnp.int32))
    )
    groups = received[order_row].reshape(slot_total // CAP, CAP, rows, kmers)
    read_onehot = (read_block[None, :] == jnp.arange(RB_DEV, dtype=jnp.int32)[:, None]).astype(
        jnp.bfloat16
    )
    others_table = np.array(
        [[column for column in range(CAP) if column != spot] for spot in range(CAP)], dtype=np.int32
    )
    ordered_partners = groups[:, others_table].reshape(slot_total, CAP - 1, rows, kmers)
    partners = ordered_partners[place_of]
    spot_send = (place_of % CAP).astype(jnp.bfloat16)[:, None]
    returned, spot_back = (
        lax.all_to_all(partners, "dev", split_axis=0, concat_axis=0, tiled=True),
        lax.all_to_all(spot_send, "dev", split_axis=0, concat_axis=0, tiled=True),
    )
    partner_blocks = jnp.einsum(
        "bs,sjrk->bjrk", onehot, returned, preferred_element_type=jnp.float32
    ).astype(jnp.bfloat16)
    spot_value = jnp.dot(onehot, spot_back, preferred_element_type=jnp.float32)[:, 0]
    spot_index = (spot_value + 0.5).astype(jnp.int32)
    stacked = []
    for column in range(CAP):
        below_pick = partner_blocks[:, min(column, CAP - 2)]
        above_pick = partner_blocks[:, max(column - 1, 0)]
        chosen = jnp.where(
            (spot_index == column)[:, None, None],
            occurrence,
            jnp.where((spot_index > column)[:, None, None], below_pick, above_pick),
        )
        stacked.append(chosen)
    partner_full = jnp.stack(stacked, axis=1)
    tile_block = jnp.einsum(
        "bik,bjrk->bijr", occurrence, partner_full, preferred_element_type=jnp.float32
    )
    tile_block = tile_block.astype(jnp.bfloat16).reshape(blocks, rows, CAP * rows)
    summed = jnp.einsum("nb,bic->nic", read_onehot, tile_block, preferred_element_type=jnp.float32)
    return summed.reshape(RB_DEV * rows, CAP * rows)


def i32(x):
    return x.astype(jnp.int32)


def iota(*shape, axis):
    return lax.broadcasted_iota(jnp.int32, shape, axis)


def group_table(block_owner, slot_order):
    devices = lax.axis_size("dev")
    blocks = block_owner.shape[0]
    slots = slot_order.shape[1]
    per_pair = slots // devices
    mine = jnp.concatenate([block_owner[:, 0], slot_order[0]])
    everyone = lax.all_gather(mine, "dev", axis=0)
    owners, order = everyone[:, :blocks], everyone[:, blocks:]
    earlier = iota(blocks, blocks, axis=1) < iota(blocks, blocks, axis=0)
    same = owners[:, :, None] == owners[:, None, :]
    rank = jnp.sum(i32(same & earlier[None]), axis=2)
    key = owners * per_pair + rank
    number = iota(devices, blocks, axis=0) * blocks + iota(devices, blocks, axis=1) + 1
    hit = key[:, :, None] == iota(1, 1, slots, axis=2)
    holder = jnp.sum(jnp.where(hit, number[:, :, None], 0), axis=1)
    holder = holder.reshape(devices, devices, per_pair).transpose(1, 0, 2).reshape(devices, slots)
    turned = order.reshape(devices, slots // CAP, CAP).transpose(2, 0, 1)
    hit = turned[:, :, :, None] == iota(1, 1, 1, slots, axis=3)
    table = jnp.sum(jnp.where(hit, holder[None, :, None, :], 0), axis=3)
    return table.reshape(CAP, devices * slots // CAP)


def fullest_lane(table, blocks):
    devices = lax.axis_size("dev")
    source = jnp.where(table > 0, (table - 1) // blocks, -1)
    named = source[:, :, None] == iota(1, 1, devices, axis=2)
    held = jnp.sum(i32(named), axis=0)
    held_chip = jnp.sum(held.reshape(-1, devices // CORES, CORES), axis=2)
    demand = jnp.einsum(
        "gc,gd->cd",
        held_chip.astype(jnp.bfloat16),
        (held > 0).astype(jnp.bfloat16),
        preferred_element_type=jnp.float32,
    )
    chips = devices // CORES
    away = iota(chips, devices, axis=0) != iota(chips, devices, axis=1) // CORES
    return jnp.max(jnp.where(away, demand, 0.0))


def routes(table, blocks, lane):
    devices = lax.axis_size("dev")
    chips = devices // CORES
    pair = CORES * blocks
    me = lax.axis_index("dev")
    chip, core = me // CORES, me % CORES
    ids = chip * pair + iota(pair, 1, axis=0) + 1
    inside = (table[0][None] == ids) | (table[1][None] == ids)
    for j in range(2, CAP):
        inside = inside | (table[j][None] == ids)
    partners = jnp.stack(
        [jnp.sum(jnp.where(inside, table[j][None], 0), axis=1) for j in range(CAP)]
    )
    source = jnp.where(partners > 0, (partners - 1) // blocks, -1)
    named = source[:, :, None] == iota(1, 1, devices, axis=2)
    need = jnp.any(named, axis=0) & (iota(1, devices, axis=1) // CORES != chip)
    before = (iota(pair, pair, axis=1) < iota(pair, pair, axis=0)).astype(jnp.bfloat16)
    rank = i32(jnp.dot(before, need.astype(jnp.bfloat16), preferred_element_type=jnp.float32))
    rank = jnp.where(need, rank, -1).T
    x = jnp.arange(pair, dtype=jnp.int32)
    local = jnp.where(x // blocks == core, x % blocks, blocks + x % blocks)
    turn = iota(1, lane, 1, axis=1) * CORES + core
    send = jnp.sum(jnp.where(rank[:, None, :] == turn, local[None, None, :], 0), axis=2)

    own = lax.dynamic_slice(partners, (0, core * blocks), (CAP, blocks)).reshape(-1)
    total = devices * blocks
    match = own[:, None] == iota(1, total, axis=1) + 1
    wanted = jnp.any(match, axis=0).reshape(chips, pair)
    arrived = i32(
        jnp.dot(wanted.astype(jnp.bfloat16), before.T, preferred_element_type=jnp.float32)
    )
    c = iota(chips, pair, axis=0)
    there = pair + (c * CORES + arrived % CORES) * lane + arrived // CORES
    place = jnp.where(c == chip, local[None, :], there).reshape(1, total)
    empty = pair + devices * lane
    pick = jnp.sum(jnp.where(match, place, 0), axis=1)
    pick = jnp.where(own > 0, pick, empty)
    return send.reshape(-1), pick


def pack_kernel(send_ref, own_ref, sib_ref, out_ref, held, sems):
    blocks = own_ref.shape[0]
    first = pltpu.make_async_copy(own_ref, held.at[pl.ds(0, blocks)], sems.at[0])
    second = pltpu.make_async_copy(sib_ref, held.at[pl.ds(blocks, blocks)], sems.at[1])
    first.start()
    second.start()
    first.wait()
    second.wait()

    def step(i, _):
        out_ref[i] = held[send_ref[i]]
        return 0

    lax.fori_loop(0, out_ref.shape[0], step, 0, unroll=4)


def tile_kernel(pick_ref, read_ref, own_ref, sib_ref, got_ref, out_ref, held, sems):
    blocks = own_ref.shape[0]
    rows = own_ref.shape[1]
    many = got_ref.shape[0]
    copies = [
        pltpu.make_async_copy(own_ref, held.at[pl.ds(0, blocks)], sems.at[0]),
        pltpu.make_async_copy(sib_ref, held.at[pl.ds(blocks, blocks)], sems.at[1]),
        pltpu.make_async_copy(got_ref, held.at[pl.ds(2 * blocks, many)], sems.at[2]),
    ]
    for copy in copies:
        copy.start()
    held[2 * blocks + many] = jnp.zeros(held.shape[1:], held.dtype)
    out_ref[...] = jnp.zeros_like(out_ref)
    for copy in copies:
        copy.wait()

    def step(b, _):
        others = jnp.concatenate([held[pick_ref[j * blocks + b]] for j in range(CAP)], axis=0)
        tile = lax.dot_general(
            held[b], others, (((1,), (1,)), ((), ())), preferred_element_type=jnp.float32
        )
        where = pl.ds(pl.multiple_of(read_ref[b] * rows, rows), rows)
        out_ref[where, :] += tile.astype(jnp.bfloat16).astype(jnp.float32)
        return 0

    lax.fori_loop(0, blocks, step, 0, unroll=2)


def direct(occurrence, sibling, read_block, table, lane):
    devices = lax.axis_size("dev")
    blocks, rows, kmers = occurrence.shape
    many = devices * lane
    send, pick = routes(table, blocks, lane)
    smem = pl.BlockSpec(memory_space=pltpu.SMEM)
    hbm = pl.BlockSpec(memory_space=pl.ANY)
    vmem = pl.BlockSpec(memory_space=pltpu.VMEM)
    outgoing = pl.pallas_call(
        pack_kernel,
        out_shape=jax.ShapeDtypeStruct((many, rows, kmers), occurrence.dtype),
        in_specs=[smem, hbm, hbm],
        out_specs=vmem,
        scratch_shapes=[
            pltpu.VMEM((CORES * blocks, rows, kmers), occurrence.dtype),
            pltpu.SemaphoreType.DMA((2,)),
        ],
        compiler_params=pltpu.CompilerParams(vmem_limit_bytes=60 << 20),
        name="pack",
    )(send, occurrence, sibling)
    incoming = lax.all_to_all(outgoing, "dev", split_axis=0, concat_axis=0, tiled=True)
    return pl.pallas_call(
        tile_kernel,
        out_shape=jax.ShapeDtypeStruct((RB_DEV * rows, CAP * rows), jnp.float32),
        in_specs=[smem, smem, hbm, hbm, hbm],
        out_specs=vmem,
        scratch_shapes=[
            pltpu.VMEM((CORES * blocks + many + 1, rows, kmers), occurrence.dtype),
            pltpu.SemaphoreType.DMA((3,)),
        ],
        compiler_params=pltpu.CompilerParams(vmem_limit_bytes=60 << 20),
        name="tiles",
    )(pick, read_block, occurrence, sibling, incoming)


def shards(occurrence, block_owner, read_block, slot_order):
    devices = lax.axis_size("dev")
    blocks = occurrence.shape[0]
    lane = 2 * (2 * blocks // devices) + 2
    swap = [(d, d ^ 1) for d in range(devices)]
    sibling = lax.ppermute(occurrence, "dev", swap)
    table = group_table(block_owner, slot_order)
    fits = fullest_lane(table, blocks) <= CORES * lane
    return lax.cond(
        fits,
        lambda: direct(occurrence, sibling, read_block, table, lane),
        lambda: exchange_by_owner(occurrence, block_owner, read_block, slot_order),
    )


def solution(mesh):
    placed = (P("dev", None, None), P("dev", None), P("dev"), P("dev", None))
    return jax.shard_map(
        shards, mesh=mesh, in_specs=placed, out_specs=P("dev", None), check_vma=False
    )
```

```python
import functools
import jax
import jax.numpy as jnp
import numpy as np
from jax import lax
from jax.experimental import pallas as pl
from jax.experimental.pallas import tpu as pltpu
from jax.sharding import PartitionSpec as P

CAP = 4
RB_DEV = 16
CORES = 2
HALVES = 2
FAMILY = CORES * HALVES


def i32(x):
    return x.astype(jnp.int32)


def iota(*shape, axis):
    return lax.broadcasted_iota(jnp.int32, shape, axis)


def group_table(block_owner, slot_order):
    devices = lax.axis_size("dev")
    blocks = block_owner.shape[0]
    slots = slot_order.shape[1]
    per_pair = slots // devices
    mine = jnp.concatenate([block_owner[:, 0], slot_order[0]])
    everyone = lax.all_gather(mine, "dev", axis=0)
    owners, order = everyone[:, :blocks], everyone[:, blocks:]
    earlier = iota(blocks, blocks, axis=1) < iota(blocks, blocks, axis=0)
    same = owners[:, :, None] == owners[:, None, :]
    rank = jnp.sum(i32(same & earlier[None]), axis=2)
    key = owners * per_pair + rank
    number = iota(devices, blocks, axis=0) * blocks + iota(devices, blocks, axis=1) + 1
    hit = key[:, :, None] == iota(1, 1, slots, axis=2)
    holder = jnp.sum(jnp.where(hit, number[:, :, None], 0), axis=1)
    holder = holder.reshape(devices, devices, per_pair).transpose(1, 0, 2).reshape(devices, slots)
    turned = order.reshape(devices, slots // CAP, CAP).transpose(2, 0, 1)
    hit = turned[:, :, :, None] == iota(1, 1, 1, slots, axis=3)
    table = jnp.sum(jnp.where(hit, holder[None, :, None, :], 0), axis=3)
    return table.reshape(CAP, devices * slots // CAP)


def fullest_lane(table, blocks):
    devices = lax.axis_size("dev")
    families = devices // FAMILY
    source = jnp.where(table > 0, (table - 1) // blocks, -1)
    named = source[:, :, None] == iota(1, 1, devices, axis=2)
    held = jnp.sum(i32(named), axis=0)
    held_family = jnp.sum(held.reshape(-1, HALVES, families, CORES), axis=(1, 3))
    demand = jnp.einsum(
        "gf,gd->fd",
        held_family.astype(jnp.bfloat16),
        (held > 0).astype(jnp.bfloat16),
        preferred_element_type=jnp.float32,
    )
    f, d = iota(families, devices, axis=0), iota(families, devices, axis=1)
    return jnp.max(jnp.where(f != d // CORES % families, demand, 0.0))


def routes(table, blocks, lane):
    devices = lax.axis_size("dev")
    families = devices // FAMILY
    half_devices = devices // HALVES
    many = FAMILY * blocks
    me = lax.axis_index("dev")
    half, family, core = me // half_devices, me // CORES % families, me % CORES
    x = jnp.arange(many, dtype=jnp.int32)
    x_half, x_core, x_block = x // (CORES * blocks), x // blocks % CORES, x % blocks
    ids = (((x_half * families + family) * CORES + x_core) * blocks + x_block + 1)[:, None]
    inside = (table[0][None] == ids) | (table[1][None] == ids)
    for j in range(2, CAP):
        inside = inside | (table[j][None] == ids)
    partners = jnp.stack(
        [jnp.sum(jnp.where(inside, table[j][None], 0), axis=1) for j in range(CAP)]
    )
    source = jnp.where(partners > 0, (partners - 1) // blocks, -1)
    target = iota(1, half_devices, axis=1) + half * half_devices
    named = source[:, :, None] == target[None]
    need = jnp.any(named, axis=0) & (target // CORES % families != family)
    before = (iota(many, many, axis=1) < iota(many, many, axis=0)).astype(jnp.bfloat16)
    rank = i32(jnp.dot(before, need.astype(jnp.bfloat16), preferred_element_type=jnp.float32))
    rank = jnp.where(need, rank, -1).T
    local = (i32(x_half != half) * CORES + i32(x_core != core)) * blocks + x_block

    begin = half * CORES * blocks + core * blocks
    own = lax.dynamic_slice(partners, (0, begin), (CAP, blocks)).reshape(-1)
    total = devices * blocks
    match = own[:, None] == iota(1, total, axis=1) + 1
    wanted = jnp.any(match, axis=0).reshape(HALVES, families, CORES * blocks)
    wanted = wanted.transpose(1, 0, 2).reshape(families, many)
    arrived = i32(
        jnp.dot(wanted.astype(jnp.bfloat16), before.T, preferred_element_type=jnp.float32)
    )
    f = iota(families, many, axis=0)
    empty = many + half_devices * lane

    def send(turn):
        spot = (turn * lane + iota(1, lane, 1, axis=1)) * CORES + core
        return jnp.sum(jnp.where(rank[:, None, :] == spot, local[None, None, :], 0), axis=2).reshape(-1)

    def pick(turn):
        now = arrived - turn * lane * CORES
        there = many + (f * CORES + now % CORES) * lane + now // CORES
        there = jnp.where((now >= 0) & (now < lane * CORES), there, empty)
        place = jnp.where(f == family, jnp.where(turn == 0, local, empty)[None, :], there)
        place = place.reshape(families, HALVES, CORES * blocks).transpose(1, 0, 2).reshape(1, total)
        found = jnp.sum(jnp.where(match, place, 0), axis=1)
        return jnp.where(own > 0, found, empty)

    return send, pick


def fill(near, held, sems):
    blocks = near[0].shape[0]
    copies = [
        pltpu.make_async_copy(ref, held.at[pl.ds(i * blocks, blocks)], sems.at[i])
        for i, ref in enumerate(near)
    ]
    for copy in copies:
        copy.start()
    return copies


def pack_kernel(send_ref, a_ref, b_ref, c_ref, d_ref, out_ref, held, sems):
    for copy in fill((a_ref, b_ref, c_ref, d_ref), held, sems):
        copy.wait()

    def step(i, _):
        out_ref[i] = held[send_ref[i]]
        return 0

    lax.fori_loop(0, out_ref.shape[0], step, 0, unroll=4)


def tile_kernel(pick_ref, read_ref, a_ref, b_ref, c_ref, d_ref, got_ref, out_ref, held, sems):
    blocks, rows = a_ref.shape[:2]
    near, many = FAMILY * blocks, got_ref.shape[0]
    copies = fill((a_ref, b_ref, c_ref, d_ref), held, sems)
    last = pltpu.make_async_copy(got_ref, held.at[pl.ds(near, many)], sems.at[FAMILY])
    last.start()
    held[near + many] = jnp.zeros(held.shape[1:], held.dtype)
    out_ref[...] = jnp.zeros_like(out_ref)
    for copy in copies:
        copy.wait()
    last.wait()

    def step(b, _):
        others = jnp.concatenate([held[pick_ref[j * blocks + b]] for j in range(CAP)], axis=0)
        tile = lax.dot_general(
            held[b], others, (((1,), (1,)), ((), ())), preferred_element_type=jnp.float32
        )
        where = pl.ds(pl.multiple_of(read_ref[b] * rows, rows), rows)
        out_ref[where, :] += tile.astype(jnp.bfloat16).astype(jnp.float32)
        return 0

    lax.fori_loop(0, blocks, step, 0, unroll=2)


SMEM = pl.BlockSpec(memory_space=pltpu.SMEM)
HBM = pl.BlockSpec(memory_space=pl.ANY)
VMEM = pl.BlockSpec(memory_space=pltpu.VMEM)


def pack(send, near):
    blocks, rows, kmers = near[0].shape
    return pl.pallas_call(
        pack_kernel,
        out_shape=jax.ShapeDtypeStruct((send.shape[0], rows, kmers), near[0].dtype),
        in_specs=[SMEM] + [HBM] * FAMILY,
        out_specs=VMEM,
        scratch_shapes=[
            pltpu.VMEM((FAMILY * blocks, rows, kmers), near[0].dtype),
            pltpu.SemaphoreType.DMA((FAMILY,)),
        ],
        compiler_params=pltpu.CompilerParams(vmem_limit_bytes=60 << 20),
        name="pack",
    )(send, *near)


def tiles(pick, read_block, near, got):
    blocks, rows, kmers = near[0].shape
    return pl.pallas_call(
        tile_kernel,
        out_shape=jax.ShapeDtypeStruct((RB_DEV * rows, CAP * rows), jnp.float32),
        in_specs=[SMEM, SMEM] + [HBM] * (FAMILY + 1),
        out_specs=VMEM,
        scratch_shapes=[
            pltpu.VMEM((FAMILY * blocks + got.shape[0] + 1, rows, kmers), got.dtype),
            pltpu.SemaphoreType.DMA((FAMILY + 1,)),
        ],
        compiler_params=pltpu.CompilerParams(vmem_limit_bytes=60 << 20),
        name="tiles",
    )(pick, read_block, *near, got)


def shards(occurrence, block_owner, read_block, slot_order):
    devices = lax.axis_size("dev")
    blocks = occurrence.shape[0]
    half_devices = devices // HALVES
    lane = 2 * (2 * blocks // devices) + 7
    swap = [(d, d ^ 1) for d in range(devices)]
    across = [(d, (d + half_devices) % devices) for d in range(devices)]
    groups = np.arange(devices).reshape(HALVES, half_devices).tolist()
    far = lax.ppermute(occurrence, "dev", across)
    sibling = lax.ppermute(occurrence, "dev", swap)
    near = (occurrence, sibling, far, lax.ppermute(far, "dev", swap))
    table = group_table(block_owner, slot_order)
    most = i32(fullest_lane(table, blocks))
    turns = (most + CORES * lane - 1) // (CORES * lane)
    send, pick = routes(table, blocks, lane)

    def one(turn):
        out = pack(send(turn), near)
        got = lax.all_to_all(
            out, "dev", split_axis=0, concat_axis=0, axis_index_groups=groups, tiled=True
        )
        return tiles(pick(turn), read_block, near, got)

    def more(carry):
        turn, margin = carry
        return turn + 1, margin + one(turn)

    first = one(jnp.int32(0))
    return lax.while_loop(lambda carry: carry[0] < turns, more, (jnp.int32(1), first))[1]


def solution(mesh):
    placed = (P("dev", None, None), P("dev", None), P("dev"), P("dev", None))
    return jax.shard_map(
        shards, mesh=mesh, in_specs=placed, out_specs=P("dev", None), check_vma=False
    )
```

```python
import functools
import jax
import jax.numpy as jnp
import numpy as np
from jax import lax
from jax.experimental import pallas as pl
from jax.experimental.pallas import tpu as pltpu
from jax.sharding import PartitionSpec as P

CAP = 4
RB_DEV = 16
CORES = 2
HALVES = 2
FAMILY = CORES * HALVES


def i32(x):
    return x.astype(jnp.int32)


def iota(*shape, axis):
    return lax.broadcasted_iota(jnp.int32, shape, axis)


def group_table(owners, order):
    devices, blocks = owners.shape
    slots = order.shape[1]
    per_pair = slots // devices
    earlier = iota(blocks, blocks, axis=1) < iota(blocks, blocks, axis=0)
    same = owners[:, :, None] == owners[:, None, :]
    rank = jnp.sum(i32(same & earlier[None]), axis=2)
    key = owners * per_pair + rank
    number = iota(devices, blocks, axis=0) * blocks + iota(devices, blocks, axis=1) + 1
    hit = key[:, :, None] == iota(1, 1, slots, axis=2)
    holder = jnp.sum(jnp.where(hit, number[:, :, None], 0), axis=1)
    holder = holder.reshape(devices, devices, per_pair).transpose(1, 0, 2).reshape(devices, slots)
    turned = order.reshape(devices, slots // CAP, CAP).transpose(2, 0, 1)
    hit = turned[:, :, :, None] == iota(1, 1, 1, slots, axis=3)
    table = jnp.sum(jnp.where(hit, holder[None, :, None, :], 0), axis=3)
    return table.reshape(CAP, devices * slots // CAP)


def fullest_lane(table, blocks):
    devices = lax.axis_size("dev")
    families = devices // FAMILY
    chips = devices // CORES
    source = jnp.where(table > 0, (table - 1) // blocks, -1)
    named = source[:, :, None] == iota(1, 1, devices, axis=2)
    held = jnp.sum(i32(named), axis=0)
    held_chip = jnp.sum(held.reshape(-1, chips, CORES), axis=2)
    demand = jnp.einsum(
        "gc,gd->cd",
        held_chip.astype(jnp.bfloat16),
        (held > 0).astype(jnp.bfloat16),
        preferred_element_type=jnp.float32,
    )
    c, d = iota(chips, devices, axis=0), iota(chips, devices, axis=1)
    return jnp.max(jnp.where(c % families != d // CORES % families, demand, 0.0))


def routes(table, blocks, lane):
    devices = lax.axis_size("dev")
    families = devices // FAMILY
    half_devices = devices // HALVES
    many = FAMILY * blocks
    me = lax.axis_index("dev")
    half, family, core = me // half_devices, me // CORES % families, me % CORES
    x = jnp.arange(many, dtype=jnp.int32)
    x_half, x_core, x_block = x // (CORES * blocks), x // blocks % CORES, x % blocks
    ids = (((x_half * families + family) * CORES + x_core) * blocks + x_block + 1)[:, None]
    inside = (table[0][None] == ids) | (table[1][None] == ids)
    for j in range(2, CAP):
        inside = inside | (table[j][None] == ids)
    partners = jnp.stack(
        [jnp.sum(jnp.where(inside, table[j][None], 0), axis=1) for j in range(CAP)]
    )
    source = jnp.where(partners > 0, (partners - 1) // blocks, -1)
    target = iota(1, half_devices, axis=1) + half * half_devices
    named = source[:, :, None] == target[None]
    need = jnp.any(named, axis=0) & (target // CORES % families != family)
    row, column = iota(many, many, axis=0), iota(many, many, axis=1)
    same_chip = row // (CORES * blocks) == column // (CORES * blocks)
    before = ((column < row) & same_chip).astype(jnp.bfloat16)
    rank = i32(jnp.dot(before, need.astype(jnp.bfloat16), preferred_element_type=jnp.float32))
    rank = jnp.where(need, rank, -1).T
    local = (i32(x_half != half) * CORES + i32(x_core != core)) * blocks + x_block

    begin = half * CORES * blocks + core * blocks
    own = lax.dynamic_slice(partners, (0, begin), (CAP, blocks)).reshape(-1)
    total = devices * blocks
    match = own[:, None] == iota(1, total, axis=1) + 1
    wanted = jnp.any(match, axis=0).reshape(HALVES, families, CORES * blocks)
    wanted = wanted.transpose(1, 0, 2).reshape(families, many)
    arrived = i32(
        jnp.dot(wanted.astype(jnp.bfloat16), before.T, preferred_element_type=jnp.float32)
    )
    f = iota(families, many, axis=0)
    part = i32(iota(families, many, axis=1) // (CORES * blocks) != half)
    empty = many + HALVES * half_devices * lane

    def send(turn, far):
        spot = (turn * lane + iota(1, lane, 1, axis=1)) * CORES + core
        chosen = jnp.where((x_half != half) == far, local % (CORES * blocks), 0)
        hit = (rank[:, None, :] == spot) & ((x_half != half) == far)
        return jnp.sum(jnp.where(hit, chosen[None, None, :], 0), axis=2).reshape(-1)

    def pick(turn):
        now = arrived - turn * lane * CORES
        there = (part * half_devices + f * CORES + now % CORES) * lane + now // CORES + many
        there = jnp.where((now >= 0) & (now < lane * CORES), there, empty)
        place = jnp.where(f == family, jnp.where(turn == 0, local, empty)[None, :], there)
        place = place.reshape(families, HALVES, CORES * blocks).transpose(1, 0, 2).reshape(1, total)
        found = jnp.sum(jnp.where(match, place, 0), axis=1)
        return jnp.where(own > 0, found, empty)

    return send, pick


def fill(near, held, sems):
    blocks = near[0].shape[0]
    copies = [
        pltpu.make_async_copy(ref, held.at[pl.ds(i * blocks, blocks)], sems.at[i])
        for i, ref in enumerate(near)
    ]
    for copy in copies:
        copy.start()
    return copies


def pack_kernel(send_ref, a_ref, b_ref, out_ref, held, sems):
    for copy in fill((a_ref, b_ref), held, sems):
        copy.wait()

    def step(i, _):
        out_ref[i] = held[send_ref[i]]
        return 0

    lax.fori_loop(0, out_ref.shape[0], step, 0, unroll=4)


def tile_kernel(pick_ref, read_ref, *refs):
    near, got, (out_ref, held, sems) = refs[:FAMILY], refs[FAMILY:-3], refs[-3:]
    blocks, rows = near[0].shape[:2]
    base, many = FAMILY * blocks, got[0].shape[0]
    copies = fill(near, held, sems)
    for i, ref in enumerate(got):
        into = held.at[pl.ds(base + i * many, many)]
        copies.append(pltpu.make_async_copy(ref, into, sems.at[FAMILY + i]))
        copies[-1].start()
    held[base + HALVES * many] = jnp.zeros(held.shape[1:], held.dtype)
    out_ref[...] = jnp.zeros_like(out_ref)
    for copy in copies:
        copy.wait()

    def step(b, _):
        others = jnp.concatenate([held[pick_ref[j * blocks + b]] for j in range(CAP)], axis=0)
        tile = lax.dot_general(
            held[b], others, (((1,), (1,)), ((), ())), preferred_element_type=jnp.float32
        )
        where = pl.ds(pl.multiple_of(read_ref[b] * rows, rows), rows)
        out_ref[where, :] += tile.astype(jnp.bfloat16).astype(jnp.float32)
        return 0

    lax.fori_loop(0, blocks, step, 0, unroll=2)


SMEM = pl.BlockSpec(memory_space=pltpu.SMEM)
HBM = pl.BlockSpec(memory_space=pl.ANY)
VMEM = pl.BlockSpec(memory_space=pltpu.VMEM)


def pack(send, near):
    blocks, rows, kmers = near[0].shape
    return pl.pallas_call(
        pack_kernel,
        out_shape=jax.ShapeDtypeStruct((send.shape[0], rows, kmers), near[0].dtype),
        in_specs=[SMEM] + [HBM] * CORES,
        out_specs=VMEM,
        scratch_shapes=[
            pltpu.VMEM((CORES * blocks, rows, kmers), near[0].dtype),
            pltpu.SemaphoreType.DMA((CORES,)),
        ],
        compiler_params=pltpu.CompilerParams(vmem_limit_bytes=60 << 20),
        name="pack",
    )(send, *near)


def tiles(pick, read_block, near, got):
    blocks, rows, kmers = near[0].shape
    total = FAMILY * blocks + HALVES * got[0].shape[0] + 1
    return pl.pallas_call(
        tile_kernel,
        out_shape=jax.ShapeDtypeStruct((RB_DEV * rows, CAP * rows), jnp.float32),
        in_specs=[SMEM, SMEM] + [HBM] * (FAMILY + HALVES),
        out_specs=VMEM,
        scratch_shapes=[
            pltpu.VMEM((total, rows, kmers), near[0].dtype),
            pltpu.SemaphoreType.DMA((FAMILY + HALVES,)),
        ],
        compiler_params=pltpu.CompilerParams(vmem_limit_bytes=60 << 20),
        name="tiles",
    )(pick, read_block, *near, *got)


def everyone_kernel(devices, row_ref, out_ref, send_sems, recv_sems):
    me = lax.axis_index("dev")
    out_ref[me] = row_ref[...]
    copies = []
    for k in range(1, devices):
        copies.append(
            pltpu.make_async_remote_copy(
                src_ref=row_ref,
                dst_ref=out_ref.at[me],
                send_sem=send_sems.at[k],
                recv_sem=recv_sems.at[k],
                device_id=(lax.rem(me + k, devices),),
                device_id_type=pl.DeviceIdType.MESH,
            )
        )
        copies[-1].start()
    for copy in copies:
        copy.wait()


def gather_rows(row):
    devices = lax.axis_size("dev")
    return pl.pallas_call(
        functools.partial(everyone_kernel, devices),
        out_shape=jax.ShapeDtypeStruct((devices,) + row.shape, row.dtype),
        in_specs=[VMEM],
        out_specs=VMEM,
        scratch_shapes=[pltpu.SemaphoreType.DMA((devices,))] * 2,
        compiler_params=pltpu.CompilerParams(has_side_effects=True),
        name="gather_rows",
    )(row)


def flipped(value, mask):
    bit = 1
    while bit <= mask:
        if mask & bit:
            value = value + bit - 2 * bit * (value // bit % 2)
        bit *= 2
    return value


def exchange_kernel(devices, lane, out_ref, got_ref, send_sems, recv_sems):
    me = lax.axis_index("dev")
    count = devices // HALVES
    spot = me % count
    copies = []
    for k in range(CORES, count):
        to = flipped(spot, k)
        copies.append(
            pltpu.make_async_remote_copy(
                src_ref=out_ref.at[pl.ds(to * lane, lane)],
                dst_ref=got_ref.at[pl.ds(spot * lane, lane)],
                send_sem=send_sems.at[k],
                recv_sem=recv_sems.at[k],
                device_id=(me - spot + to,),
                device_id_type=pl.DeviceIdType.MESH,
            )
        )
        copies[-1].start()
    for copy in copies:
        copy.wait()


def exchange(out, lane):
    devices = lax.axis_size("dev")
    count = devices // HALVES
    return pl.pallas_call(
        functools.partial(exchange_kernel, devices, lane),
        out_shape=jax.ShapeDtypeStruct(out.shape, out.dtype),
        in_specs=[HBM],
        out_specs=HBM,
        scratch_shapes=[pltpu.SemaphoreType.DMA((count,))] * 2,
        compiler_params=pltpu.CompilerParams(has_side_effects=True),
        cost_estimate=pl.CostEstimate(
            flops=0, bytes_accessed=32 * out.size * out.dtype.itemsize, transcendentals=0
        ),
        name="exchange",
    )(out)


def shards(occurrence, block_owner, read_block, slot_order):
    devices = lax.axis_size("dev")
    blocks = occurrence.shape[0]
    slots = slot_order.shape[1]
    lane = 2 * (2 * blocks // devices) + 1
    swap = [(d, d ^ 1) for d in range(devices)]
    across = [(d, (d + devices // HALVES) % devices) for d in range(devices)]
    row = jnp.stack([jnp.pad(block_owner[:, 0], (0, slots - blocks)), slot_order[0]])
    everyone = gather_rows(row)
    everyone, mine = lax.optimization_barrier((everyone, occurrence))
    far = lax.ppermute(mine, "dev", across)
    sibling = lax.ppermute(mine, "dev", swap)
    table = group_table(everyone[:, 0, :blocks], everyone[:, 1])
    most = i32(fullest_lane(table, blocks))
    turns = (most + CORES * lane - 1) // (CORES * lane)
    send, pick = routes(table, blocks, lane)
    got = exchange(pack(send(0, False), (occurrence, sibling)), lane)
    far, got = lax.optimization_barrier((far, got))
    distant = (far, lax.ppermute(far, "dev", swap))
    near = (occurrence, sibling) + distant
    also = exchange(pack(send(0, True), distant), lane)
    first = tiles(pick(0), read_block, near, (got, also))

    def more(carry):
        turn, margin = carry
        got = exchange(pack(send(turn, False), near[:CORES]), lane)
        also = exchange(pack(send(turn, True), distant), lane)
        return turn + 1, margin + tiles(pick(turn), read_block, near, (got, also))

    return lax.while_loop(lambda carry: carry[0] < turns, more, (jnp.int32(1), first))[1]


def solution(mesh):
    placed = (P("dev", None, None), P("dev", None), P("dev"), P("dev", None))
    return jax.shard_map(
        shards, mesh=mesh, in_specs=placed, out_specs=P("dev", None), check_vma=False
    )
```

```python
import functools
import jax
import jax.numpy as jnp
import numpy as np
from jax import lax
from jax.experimental import pallas as pl
from jax.experimental.pallas import tpu as pltpu
from jax.sharding import PartitionSpec as P

CAP = 4
RB_DEV = 16
CORES = 2
HALVES = 2
FAMILY = CORES * HALVES


def i32(x):
    return x.astype(jnp.int32)


def iota(*shape, axis):
    return lax.broadcasted_iota(jnp.int32, shape, axis)


def group_table(owners, order):
    devices, blocks = owners.shape
    slots = order.shape[1]
    per_pair = slots // devices
    earlier = iota(blocks, blocks, axis=1) < iota(blocks, blocks, axis=0)
    same = owners[:, :, None] == owners[:, None, :]
    rank = jnp.sum(i32(same & earlier[None]), axis=2)
    key = owners * per_pair + rank
    number = iota(devices, blocks, axis=0) * blocks + iota(devices, blocks, axis=1) + 1
    hit = key[:, :, None] == iota(1, 1, slots, axis=2)
    holder = jnp.sum(jnp.where(hit, number[:, :, None], 0), axis=1)
    holder = holder.reshape(devices, devices, per_pair).transpose(1, 0, 2).reshape(devices, slots)
    turned = order.reshape(devices, slots // CAP, CAP).transpose(2, 0, 1)
    hit = turned[:, :, :, None] == iota(1, 1, 1, slots, axis=3)
    table = jnp.sum(jnp.where(hit, holder[None, :, None, :], 0), axis=3)
    return table.reshape(CAP, devices * slots // CAP)


def fullest_lane(table, blocks):
    devices = lax.axis_size("dev")
    families = devices // FAMILY
    chips = devices // CORES
    source = jnp.where(table > 0, (table - 1) // blocks, -1)
    named = source[:, :, None] == iota(1, 1, devices, axis=2)
    held = jnp.sum(i32(named), axis=0)
    held_chip = jnp.sum(held.reshape(-1, chips, CORES), axis=2)
    demand = jnp.einsum(
        "gc,gd->cd",
        held_chip.astype(jnp.bfloat16),
        (held > 0).astype(jnp.bfloat16),
        preferred_element_type=jnp.float32,
    )
    c, d = iota(chips, devices, axis=0), iota(chips, devices, axis=1)
    return jnp.max(jnp.where(c % families != d // CORES % families, demand, 0.0))


def routes(table, blocks):
    devices = lax.axis_size("dev")
    families = devices // FAMILY
    half_devices = devices // HALVES
    many = FAMILY * blocks
    me = lax.axis_index("dev")
    half, family, core = me // half_devices, me // CORES % families, me % CORES
    x = jnp.arange(many, dtype=jnp.int32)
    x_half, x_core, x_block = x // (CORES * blocks), x // blocks % CORES, x % blocks
    ids = (((x_half * families + family) * CORES + x_core) * blocks + x_block + 1)[:, None]
    inside = (table[0][None] == ids) | (table[1][None] == ids)
    for j in range(2, CAP):
        inside = inside | (table[j][None] == ids)
    partners = jnp.stack(
        [jnp.sum(jnp.where(inside, table[j][None], 0), axis=1) for j in range(CAP)]
    )
    source = jnp.where(partners > 0, (partners - 1) // blocks, -1)
    target = iota(1, half_devices, axis=1) + half * half_devices
    named = source[:, :, None] == target[None]
    need = jnp.any(named, axis=0) & (target // CORES % families != family)
    row, column = iota(many, many, axis=0), iota(many, many, axis=1)
    same_chip = row // (CORES * blocks) == column // (CORES * blocks)
    before = ((column < row) & same_chip).astype(jnp.bfloat16)
    rank = i32(jnp.dot(before, need.astype(jnp.bfloat16), preferred_element_type=jnp.float32))
    rank = jnp.where(need, rank, -1).T
    local = (i32(x_half != half) * CORES + i32(x_core != core)) * blocks + x_block

    begin = half * CORES * blocks + core * blocks
    own = lax.dynamic_slice(partners, (0, begin), (CAP, blocks)).reshape(-1)
    total = devices * blocks
    match = own[:, None] == iota(1, total, axis=1) + 1
    wanted = jnp.any(match, axis=0).reshape(HALVES, families, CORES * blocks)
    wanted = wanted.transpose(1, 0, 2).reshape(families, many)
    arrived = i32(
        jnp.dot(wanted.astype(jnp.bfloat16), before.T, preferred_element_type=jnp.float32)
    )
    f = iota(families, many, axis=0)
    part = i32(iota(families, many, axis=1) // (CORES * blocks) != half)

    def send(begin, lane, far):
        spot = begin + iota(1, lane, 1, axis=1) * CORES + core
        chosen = jnp.where((x_half != half) == far, local % (CORES * blocks), 0)
        hit = (rank[:, None, :] == spot) & ((x_half != half) == far)
        return jnp.sum(jnp.where(hit, chosen[None, None, :], 0), axis=2).reshape(-1)

    def pick(begin, lane, local):
        empty = many + HALVES * half_devices * lane
        now = arrived - begin
        there = (part * half_devices + f * CORES + now % CORES) * lane + now // CORES + many
        there = jnp.where((now >= 0) & (now < lane * CORES), there, empty)
        place = jnp.where(f == family, empty if local is None else local[None, :], there)
        place = place.reshape(families, HALVES, CORES * blocks).transpose(1, 0, 2).reshape(1, total)
        found = jnp.sum(jnp.where(match, place, 0), axis=1)
        return jnp.where(own > 0, found, empty)

    return send, pick, local


def fill(near, held, sems):
    blocks = near[0].shape[0]
    copies = [
        pltpu.make_async_copy(ref, held.at[pl.ds(i * blocks, blocks)], sems.at[i])
        for i, ref in enumerate(near)
    ]
    for copy in copies:
        copy.start()
    return copies


def pack_kernel(send_ref, a_ref, b_ref, out_ref, held, sems):
    for copy in fill((a_ref, b_ref), held, sems):
        copy.wait()

    def step(i, _):
        out_ref[i] = held[send_ref[i]]
        return 0

    lax.fori_loop(0, out_ref.shape[0], step, 0, unroll=4)


def tile_kernel(pick_ref, read_ref, *refs):
    near, got, (out_ref, held, sems) = refs[:FAMILY], refs[FAMILY:-3], refs[-3:]
    blocks, rows = near[0].shape[:2]
    base, many = FAMILY * blocks, got[0].shape[0]
    copies = fill(near, held, sems)
    for i, ref in enumerate(got):
        into = held.at[pl.ds(base + i * many, many)]
        copies.append(pltpu.make_async_copy(ref, into, sems.at[FAMILY + i]))
        copies[-1].start()
    held[base + HALVES * many] = jnp.zeros(held.shape[1:], held.dtype)
    out_ref[...] = jnp.zeros_like(out_ref)
    for copy in copies:
        copy.wait()

    def step(b, _):
        others = jnp.concatenate([held[pick_ref[j * blocks + b]] for j in range(CAP)], axis=0)
        tile = lax.dot_general(
            held[b], others, (((1,), (1,)), ((), ())), preferred_element_type=jnp.float32
        )
        where = pl.ds(pl.multiple_of(read_ref[b] * rows, rows), rows)
        out_ref[where, :] += tile.astype(jnp.bfloat16).astype(jnp.float32)
        return 0

    lax.fori_loop(0, blocks, step, 0, unroll=2)


SMEM = pl.BlockSpec(memory_space=pltpu.SMEM)
HBM = pl.BlockSpec(memory_space=pl.ANY)
VMEM = pl.BlockSpec(memory_space=pltpu.VMEM)


def pack(send, near):
    blocks, rows, kmers = near[0].shape
    return pl.pallas_call(
        pack_kernel,
        out_shape=jax.ShapeDtypeStruct((send.shape[0], rows, kmers), near[0].dtype),
        in_specs=[SMEM] + [HBM] * CORES,
        out_specs=VMEM,
        scratch_shapes=[
            pltpu.VMEM((CORES * blocks, rows, kmers), near[0].dtype),
            pltpu.SemaphoreType.DMA((CORES,)),
        ],
        compiler_params=pltpu.CompilerParams(vmem_limit_bytes=60 << 20),
        name="pack",
    )(send, *near)


def tiles(pick, read_block, near, got):
    blocks, rows, kmers = near[0].shape
    total = FAMILY * blocks + HALVES * got[0].shape[0] + 1
    return pl.pallas_call(
        tile_kernel,
        out_shape=jax.ShapeDtypeStruct((RB_DEV * rows, CAP * rows), jnp.float32),
        in_specs=[SMEM, SMEM] + [HBM] * (FAMILY + HALVES),
        out_specs=VMEM,
        scratch_shapes=[
            pltpu.VMEM((total, rows, kmers), near[0].dtype),
            pltpu.SemaphoreType.DMA((FAMILY + HALVES,)),
        ],
        compiler_params=pltpu.CompilerParams(vmem_limit_bytes=60 << 20),
        name="tiles",
    )(pick, read_block, *near, *got)


def everyone_kernel(devices, group, row_ref, out_ref, send_sems, recv_sems):
    me = lax.axis_index("dev")
    first = me // group * group
    out_ref[me] = row_ref[...]

    def spread(src, dst, to, k):
        copy = pltpu.make_async_remote_copy(
            src_ref=src,
            dst_ref=dst,
            send_sem=send_sems.at[k],
            recv_sem=recv_sems.at[k],
            device_id=(to,),
            device_id_type=pl.DeviceIdType.MESH,
        )
        copy.start()
        return copy

    near = [
        spread(row_ref, out_ref.at[me], first + (me - first + k) % group, k)
        for k in range(1, group)
    ]
    for copy in near:
        copy.wait()
    rows = out_ref.at[pl.ds(first, group)]
    far = [
        spread(rows, rows, (me + k * group) % devices, group + k)
        for k in range(1, devices // group)
    ]
    for copy in far:
        copy.wait()


def gather_rows(row):
    devices = lax.axis_size("dev")
    group = 1 << devices.bit_length() // 2
    return pl.pallas_call(
        functools.partial(everyone_kernel, devices, group),
        out_shape=jax.ShapeDtypeStruct((devices,) + row.shape, row.dtype),
        in_specs=[VMEM],
        out_specs=VMEM,
        scratch_shapes=[pltpu.SemaphoreType.DMA((group + devices // group,))] * 2,
        compiler_params=pltpu.CompilerParams(has_side_effects=True),
        name="gather_rows",
    )(row)


def flipped(value, mask):
    bit = 1
    while bit <= mask:
        if mask & bit:
            value = value + bit - 2 * bit * (value // bit % 2)
        bit *= 2
    return value


def exchange_kernel(devices, lane, out_ref, got_ref, send_sems, recv_sems):
    me = lax.axis_index("dev")
    count = devices // HALVES
    spot = me % count

    def copy_of(k):
        to = flipped(spot, k)
        return pltpu.make_async_remote_copy(
            src_ref=out_ref.at[pl.ds(to * lane, lane)],
            dst_ref=got_ref.at[pl.ds(spot * lane, lane)],
            send_sem=send_sems.at[k],
            recv_sem=recv_sems.at[k],
            device_id=(me - spot + to,),
            device_id_type=pl.DeviceIdType.MESH,
        )

    chips = count // CORES
    steps = []
    for mask in range(chips - 1, chips // 2 - 1, -1):
        for core in range(CORES):
            masks = [m for m in (mask, chips - 1 - mask) if m]
            steps.append([copy_of(m * CORES + core) for m in masks])
    for i, step in enumerate(steps):
        if i >= 2:
            for copy in steps[i - 2]:
                copy.wait_send()
        for copy in step:
            copy.start()
    for step in steps[-2:]:
        for copy in step:
            copy.wait_send()
    for step in steps:
        for copy in step:
            copy.wait_recv()


def exchange(out, lane):
    devices = lax.axis_size("dev")
    count = devices // HALVES
    return pl.pallas_call(
        functools.partial(exchange_kernel, devices, lane),
        out_shape=jax.ShapeDtypeStruct(out.shape, out.dtype),
        in_specs=[HBM],
        out_specs=HBM,
        scratch_shapes=[pltpu.SemaphoreType.DMA((count,))] * 2,
        compiler_params=pltpu.CompilerParams(has_side_effects=True),
        cost_estimate=pl.CostEstimate(
            flops=0, bytes_accessed=32 * out.size * out.dtype.itemsize, transcendentals=0
        ),
        name="exchange",
    )(out)


def shards(occurrence, block_owner, read_block, slot_order):
    devices = lax.axis_size("dev")
    blocks = occurrence.shape[0]
    slots = slot_order.shape[1]
    lane = 2 * (2 * blocks // devices) + 2
    spill = 2 * blocks // devices
    swap = [(d, d ^ 1) for d in range(devices)]
    across = [(d, (d + devices // HALVES) % devices) for d in range(devices)]
    row = jnp.stack([jnp.pad(block_owner[:, 0], (0, slots - blocks)), slot_order[0]])
    everyone = gather_rows(row)
    everyone, mine = lax.optimization_barrier((everyone, occurrence))
    far = lax.ppermute(mine, "dev", across)
    sibling = lax.ppermute(mine, "dev", swap)
    table = group_table(everyone[:, 0, :blocks], everyone[:, 1])
    most = i32(fullest_lane(table, blocks))
    send, pick, local = routes(table, blocks)
    begin = CORES * lane
    got = exchange(pack(send(0, lane, False), (occurrence, sibling)), lane)
    far, got = lax.optimization_barrier((far, got))
    distant = (far, lax.ppermute(far, "dev", swap))
    near = (occurrence, sibling) + distant
    also = exchange(pack(send(0, lane, True), distant), lane)
    first = tiles(pick(0, lane, local), read_block, near, (got, also))

    def more(carry):
        begin, margin = carry
        got = exchange(pack(send(begin, spill, False), near[:CORES]), spill)
        also = exchange(pack(send(begin, spill, True), distant), spill)
        added = tiles(pick(begin, spill, None), read_block, near, (got, also))
        return begin + CORES * spill, margin + added

    return lax.while_loop(lambda carry: carry[0] < most, more, (jnp.int32(begin), first))[1]


def solution(mesh):
    placed = (P("dev", None, None), P("dev", None), P("dev"), P("dev", None))
    return jax.shard_map(
        shards, mesh=mesh, in_specs=placed, out_specs=P("dev", None), check_vma=False
    )
```

```python
import functools
import jax
import jax.numpy as jnp
import numpy as np
from jax import lax
from jax.experimental import pallas as pl
from jax.experimental.pallas import tpu as pltpu
from jax.sharding import PartitionSpec as P

CAP = 4
RB_DEV = 16
CORES = 2
HALVES = 2
FAMILY = CORES * HALVES


def i32(x):
    return x.astype(jnp.int32)


def iota(*shape, axis):
    return lax.broadcasted_iota(jnp.int32, shape, axis)


def group_table(owners, order):
    devices, blocks = owners.shape
    slots = order.shape[1]
    per_pair = slots // devices
    earlier = iota(blocks, blocks, axis=1) < iota(blocks, blocks, axis=0)
    same = owners[:, :, None] == owners[:, None, :]
    rank = jnp.sum(i32(same & earlier[None]), axis=2)
    key = owners * per_pair + rank
    number = iota(devices, blocks, axis=0) * blocks + iota(devices, blocks, axis=1) + 1
    hit = key[:, :, None] == iota(1, 1, slots, axis=2)
    holder = jnp.sum(jnp.where(hit, number[:, :, None], 0), axis=1)
    holder = holder.reshape(devices, devices, per_pair).transpose(1, 0, 2).reshape(devices, slots)
    turned = order.reshape(devices, slots // CAP, CAP).transpose(2, 0, 1)
    hit = turned[:, :, :, None] == iota(1, 1, 1, slots, axis=3)
    table = jnp.sum(jnp.where(hit, holder[None, :, None, :], 0), axis=3)
    return table.reshape(CAP, devices * slots // CAP)


def fullest_lane(table, blocks):
    devices = lax.axis_size("dev")
    families = devices // FAMILY
    chips = devices // CORES
    source = jnp.where(table > 0, (table - 1) // blocks, -1)
    named = source[:, :, None] == iota(1, 1, devices, axis=2)
    held = jnp.sum(i32(named), axis=0)
    held_chip = jnp.sum(held.reshape(-1, chips, CORES), axis=2)
    demand = jnp.einsum(
        "gc,gd->cd",
        held_chip.astype(jnp.bfloat16),
        (held > 0).astype(jnp.bfloat16),
        preferred_element_type=jnp.float32,
    )
    c, d = iota(chips, devices, axis=0), iota(chips, devices, axis=1)
    return jnp.max(jnp.where(c % families != d // CORES % families, demand, 0.0))


def routes(table, blocks):
    devices = lax.axis_size("dev")
    families = devices // FAMILY
    half_devices = devices // HALVES
    many = FAMILY * blocks
    me = lax.axis_index("dev")
    half, family, core = me // half_devices, me // CORES % families, me % CORES
    x = jnp.arange(many, dtype=jnp.int32)
    x_half, x_core, x_block = x // (CORES * blocks), x // blocks % CORES, x % blocks
    ids = (((x_half * families + family) * CORES + x_core) * blocks + x_block + 1)[:, None]
    inside = (table[0][None] == ids) | (table[1][None] == ids)
    for j in range(2, CAP):
        inside = inside | (table[j][None] == ids)
    partners = jnp.stack(
        [jnp.sum(jnp.where(inside, table[j][None], 0), axis=1) for j in range(CAP)]
    )
    source = jnp.where(partners > 0, (partners - 1) // blocks, -1)
    target = iota(1, half_devices, axis=1) + half * half_devices
    named = source[:, :, None] == target[None]
    need = jnp.any(named, axis=0) & (target // CORES % families != family)
    row, column = iota(many, many, axis=0), iota(many, many, axis=1)
    same_chip = row // (CORES * blocks) == column // (CORES * blocks)
    before = ((column < row) & same_chip).astype(jnp.bfloat16)
    rank = i32(jnp.dot(before, need.astype(jnp.bfloat16), preferred_element_type=jnp.float32))
    rank = jnp.where(need, rank, -1).T
    local = (i32(x_half != half) * CORES + i32(x_core != core)) * blocks + x_block

    begin = half * CORES * blocks + core * blocks
    own = lax.dynamic_slice(partners, (0, begin), (CAP, blocks)).reshape(-1)
    total = devices * blocks
    match = own[:, None] == iota(1, total, axis=1) + 1
    wanted = jnp.any(match, axis=0).reshape(HALVES, families, CORES * blocks)
    wanted = wanted.transpose(1, 0, 2).reshape(families, many)
    arrived = i32(
        jnp.dot(wanted.astype(jnp.bfloat16), before.T, preferred_element_type=jnp.float32)
    )
    f = iota(families, many, axis=0)
    part = i32(iota(families, many, axis=1) // (CORES * blocks) != half)

    def send(begin, lane, far):
        spot = begin + iota(1, lane, 1, axis=1) * CORES + core
        chosen = jnp.where((x_half != half) == far, local % (CORES * blocks), 0)
        hit = (rank[:, None, :] == spot) & ((x_half != half) == far)
        return jnp.sum(jnp.where(hit, chosen[None, None, :], 0), axis=2).reshape(-1)

    def pick(begin, lane, local):
        empty = many + HALVES * half_devices * lane
        now = arrived - begin
        there = (part * half_devices + f * CORES + now % CORES) * lane + now // CORES + many
        there = jnp.where((now >= 0) & (now < lane * CORES), there, empty)
        place = jnp.where(f == family, empty if local is None else local[None, :], there)
        place = place.reshape(families, HALVES, CORES * blocks).transpose(1, 0, 2).reshape(1, total)
        found = jnp.sum(jnp.where(match, place, 0), axis=1)
        return jnp.where(own > 0, found, empty)

    return send, pick, local


def fill(near, held, sems):
    blocks = near[0].shape[0]
    copies = [
        pltpu.make_async_copy(ref, held.at[pl.ds(i * blocks, blocks)], sems.at[i])
        for i, ref in enumerate(near)
    ]
    for copy in copies:
        copy.start()
    return copies


def pack_kernel(send_ref, a_ref, b_ref, out_ref, held, sems):
    for copy in fill((a_ref, b_ref), held, sems):
        copy.wait()

    def step(i, _):
        out_ref[i] = held[send_ref[i]]
        return 0

    lax.fori_loop(0, out_ref.shape[0], step, 0, unroll=4)


def tile_kernel(pick_ref, read_ref, *refs):
    near, got, (out_ref, held, sems) = refs[:FAMILY], refs[FAMILY:-3], refs[-3:]
    blocks, rows = near[0].shape[:2]
    base, many = FAMILY * blocks, got[0].shape[0]
    copies = fill(near, held, sems)
    for i, ref in enumerate(got):
        into = held.at[pl.ds(base + i * many, many)]
        copies.append(pltpu.make_async_copy(ref, into, sems.at[FAMILY + i]))
        copies[-1].start()
    held[base + HALVES * many] = jnp.zeros(held.shape[1:], held.dtype)
    out_ref[...] = jnp.zeros_like(out_ref)
    for copy in copies:
        copy.wait()

    def step(b, _):
        others = jnp.concatenate([held[pick_ref[j * blocks + b]] for j in range(CAP)], axis=0)
        tile = lax.dot_general(
            held[b], others, (((1,), (1,)), ((), ())), preferred_element_type=jnp.float32
        )
        where = pl.ds(pl.multiple_of(read_ref[b] * rows, rows), rows)
        out_ref[where, :] += tile.astype(jnp.bfloat16).astype(jnp.float32)
        return 0

    lax.fori_loop(0, blocks, step, 0, unroll=2)


SMEM = pl.BlockSpec(memory_space=pltpu.SMEM)
HBM = pl.BlockSpec(memory_space=pl.ANY)
VMEM = pl.BlockSpec(memory_space=pltpu.VMEM)


def pack(send, near):
    blocks, rows, kmers = near[0].shape
    return pl.pallas_call(
        pack_kernel,
        out_shape=jax.ShapeDtypeStruct((send.shape[0], rows, kmers), near[0].dtype),
        in_specs=[SMEM] + [HBM] * CORES,
        out_specs=VMEM,
        scratch_shapes=[
            pltpu.VMEM((CORES * blocks, rows, kmers), near[0].dtype),
            pltpu.SemaphoreType.DMA((CORES,)),
        ],
        compiler_params=pltpu.CompilerParams(vmem_limit_bytes=60 << 20),
        name="pack",
    )(send, *near)


def tiles(pick, read_block, near, got):
    blocks, rows, kmers = near[0].shape
    total = FAMILY * blocks + HALVES * got[0].shape[0] + 1
    return pl.pallas_call(
        tile_kernel,
        out_shape=jax.ShapeDtypeStruct((RB_DEV * rows, CAP * rows), jnp.float32),
        in_specs=[SMEM, SMEM] + [HBM] * (FAMILY + HALVES),
        out_specs=VMEM,
        scratch_shapes=[
            pltpu.VMEM((total, rows, kmers), near[0].dtype),
            pltpu.SemaphoreType.DMA((FAMILY + HALVES,)),
        ],
        compiler_params=pltpu.CompilerParams(vmem_limit_bytes=60 << 20),
        name="tiles",
    )(pick, read_block, *near, *got)


def everyone_kernel(devices, group, row_ref, out_ref, send_sems, recv_sems):
    me = lax.axis_index("dev")
    first = me // group * group
    out_ref[me] = row_ref[...]

    def spread(src, dst, to, k):
        copy = pltpu.make_async_remote_copy(
            src_ref=src,
            dst_ref=dst,
            send_sem=send_sems.at[k],
            recv_sem=recv_sems.at[k],
            device_id=(to,),
            device_id_type=pl.DeviceIdType.MESH,
        )
        copy.start()
        return copy

    near = [
        spread(row_ref, out_ref.at[me], first + (me - first + k) % group, k)
        for k in range(1, group)
    ]
    for copy in near:
        copy.wait()
    rows = out_ref.at[pl.ds(first, group)]
    far = [
        spread(rows, rows, (me + k * group) % devices, group + k)
        for k in range(1, devices // group)
    ]
    for copy in far:
        copy.wait()


def gather_rows(row):
    devices = lax.axis_size("dev")
    group = 1 << devices.bit_length() // 2
    return pl.pallas_call(
        functools.partial(everyone_kernel, devices, group),
        out_shape=jax.ShapeDtypeStruct((devices,) + row.shape, row.dtype),
        in_specs=[VMEM],
        out_specs=VMEM,
        scratch_shapes=[pltpu.SemaphoreType.DMA((group + devices // group,))] * 2,
        compiler_params=pltpu.CompilerParams(has_side_effects=True),
        name="gather_rows",
    )(row)


def flipped(value, mask):
    bit = 1
    while bit <= mask:
        if mask & bit:
            value = value + bit - 2 * bit * (value // bit % 2)
        bit *= 2
    return value


def exchange_kernel(devices, lane, out_ref, got_ref, send_sems, recv_sems):
    me = lax.axis_index("dev")
    count = devices // HALVES
    spot = me % count

    def copy_of(k):
        to = flipped(spot, k)
        return pltpu.make_async_remote_copy(
            src_ref=out_ref.at[pl.ds(to * lane, lane)],
            dst_ref=got_ref.at[pl.ds(spot * lane, lane)],
            send_sem=send_sems.at[k],
            recv_sem=recv_sems.at[k],
            device_id=(me - spot + to,),
            device_id_type=pl.DeviceIdType.MESH,
        )

    chips = count // CORES
    steps = []
    for mask in range(chips - 1, chips // 2 - 1, -1):
        for core in range(CORES):
            masks = [m for m in (mask, chips - 1 - mask) if m]
            steps.append([copy_of(m * CORES + core) for m in masks])
    for i, step in enumerate(steps):
        if i >= 2:
            for copy in steps[i - 2]:
                copy.wait_send()
        for copy in step:
            copy.start()
    for step in steps[-2:]:
        for copy in step:
            copy.wait_send()
    for step in steps:
        for copy in step:
            copy.wait_recv()


def exchange(out, lane):
    devices = lax.axis_size("dev")
    count = devices // HALVES
    return pl.pallas_call(
        functools.partial(exchange_kernel, devices, lane),
        out_shape=jax.ShapeDtypeStruct(out.shape, out.dtype),
        in_specs=[HBM],
        out_specs=HBM,
        scratch_shapes=[pltpu.SemaphoreType.DMA((count,))] * 2,
        compiler_params=pltpu.CompilerParams(has_side_effects=True),
        cost_estimate=pl.CostEstimate(
            flops=0, bytes_accessed=32 * out.size * out.dtype.itemsize, transcendentals=0
        ),
        name="exchange",
    )(out)


def shards(occurrence, block_owner, read_block, slot_order):
    devices = lax.axis_size("dev")
    blocks = occurrence.shape[0]
    slots = slot_order.shape[1]
    lane = 2 * (2 * blocks // devices) + 1
    spill = 2 * blocks // devices
    swap = [(d, d ^ 1) for d in range(devices)]
    across = [(d, (d + devices // HALVES) % devices) for d in range(devices)]
    row = jnp.stack([jnp.pad(block_owner[:, 0], (0, slots - blocks)), slot_order[0]])
    everyone = gather_rows(row)
    everyone, mine = lax.optimization_barrier((everyone, occurrence))
    far = lax.ppermute(mine, "dev", across)
    sibling = lax.ppermute(mine, "dev", swap)
    table = group_table(everyone[:, 0, :blocks], everyone[:, 1])
    most = i32(fullest_lane(table, blocks))
    send, pick, local = routes(table, blocks)
    begin = CORES * lane
    got = exchange(pack(send(0, lane, False), (occurrence, sibling)), lane)
    far, got = lax.optimization_barrier((far, got))
    distant = (far, lax.ppermute(far, "dev", swap))
    near = (occurrence, sibling) + distant
    also = exchange(pack(send(0, lane, True), distant), lane)
    first = tiles(pick(0, lane, local), read_block, near, (got, also))

    def more(carry):
        begin, margin = carry
        got = exchange(pack(send(begin, spill, False), near[:CORES]), spill)
        also = exchange(pack(send(begin, spill, True), distant), spill)
        added = tiles(pick(begin, spill, None), read_block, near, (got, also))
        return begin + CORES * spill, margin + added

    return lax.while_loop(lambda carry: carry[0] < most, more, (jnp.int32(begin), first))[1]


def solution(mesh):
    placed = (P("dev", None, None), P("dev", None), P("dev"), P("dev", None))
    return jax.shard_map(
        shards, mesh=mesh, in_specs=placed, out_specs=P("dev", None), check_vma=False
    )
```
